32 devices in a mesh: rep: 8 (over z, x), tp: 4 (over y, core).
Axes of the slice: x: 2, y: 2, z: 4, core: 2. Of those that a mesh axis runs over, the one named last changes fastest.
Arguments:
- q_weight: float32 [5120, 5120], P(('rep', 'tp')), may hold values from -0.078125 to 0.078125
- key_projection_weight: float32 [1024, 5120], P(('rep', 'tp')), may hold values from -0.078125 to 0.078125
- value_projection_weight: float32 [1024, 5120], P(('rep', 'tp')), may hold values from -0.078125 to 0.078125
- tokens: bfloat16 [8192, 5120], P(('rep', 'tp')), may hold values from -6 to 6
Outputs:
- combined_query_key_value: bfloat16 [7168, 5120], P('tp')
- projected: bfloat16 [8192, 7168], P('rep', 'tp')
The draws below stay inside these ranges and needn't reach their ends.
All inputs are finite; a program needn't handle non-finite values.
Results may differ from the reference program's by a relative error of at most 0.0049.
Values may be sent and summed in bfloat16 or wider, within the bound.
A program may use at most 192 MiB of HBM per device.

```python
import jax
import jax.numpy as jnp

MODEL_WIDTH = 5120
HQ = 40
KEY_VALUE_HEADS = 8
HEAD_SIZE = 128
TOKENS = 8192
N_TP = 4


def block_scale(key, shape, cuts, smallest, top_value):
    level, own = 1.0, jax.random.fold_in(key, 6)
    for dim, shards_of in cuts:
        heights = jnp.exp(jax.random.uniform(jax.random.fold_in(own, dim), (shards_of,), jnp.float32, smallest / len(cuts), top_value / len(cuts)))
        level = level * jnp.repeat(heights, shape[dim] // shards_of).reshape([-1 if axis == dim else 1 for axis in range(len(shape))])
    return level


def bell_draw(key, dims, width, bound, shards=(), kind=jnp.bfloat16):
    array = width * jax.random.normal(key, dims, jnp.float32)
    if shards:
        array = array * block_scale(key, dims, shards, -0.22, 0.18)
    return jnp.clip(array, -bound, bound).astype(kind)


def setup_inputs(seed: int = 0) -> dict:
    seeds = jax.random.split(jax.random.key(seed), 5)
    return {
        "q_weight": bell_draw(seeds[0], (HQ * HEAD_SIZE, MODEL_WIDTH), MODEL_WIDTH ** -0.5, 0.078125, ((0, 32),), jnp.float32),
        "key_projection_weight": bell_draw(seeds[1], (KEY_VALUE_HEADS * HEAD_SIZE, MODEL_WIDTH), MODEL_WIDTH ** -0.5, 0.078125, ((0, 32),), jnp.float32),
        "value_projection_weight": bell_draw(seeds[2], (KEY_VALUE_HEADS * HEAD_SIZE, MODEL_WIDTH), MODEL_WIDTH ** -0.5, 0.078125, ((0, 32),), jnp.float32),
        "tokens": bell_draw(seeds[3], (TOKENS, MODEL_WIDTH), 1.0, 6.0, ((0, 32),)),
    }


def reference(q_weight, key_projection_weight, value_projection_weight, tokens):
    blocks = []
    for source in (q_weight, key_projection_weight, value_projection_weight):
        rounded = source.astype(jnp.bfloat16)
        blocks.append(rounded.reshape(N_TP, -1, MODEL_WIDTH))
    combined_query_key_value = jnp.concatenate(blocks, axis=1).reshape(-1, MODEL_WIDTH)
    projected = jnp.dot(tokens, combined_query_key_value.T, preferred_element_type=jnp.float32).astype(jnp.bfloat16)
    return combined_query_key_value, projected
```

```python
import functools

import jax
import jax.numpy as jnp
from jax import lax
from jax.experimental import pallas as pl
from jax.experimental.pallas import tpu as pltpu
from jax.sharding import PartitionSpec as P

MESH = pl.DeviceIdType.MESH
LEAD = 4
Y_LAG = 3
LATE_FIRST = (4, 2)
LATE_RATE = (6, 5)
TOK_FIRST = 2
TOK_AT = 8
TOK_RATE = 2
TOK_CHUNKS = 8
TWIN_AT = 18
TWIN_RATE = 4
FAR_AT = 24
MEET_AT = 24
FIRST_AT = (99, 99)
TWICE = (17, 28)
TILE = 256
VMEM = 16


def order_of(columns, tp_size, q_rows, kv_rows, column, side):
    block = columns * tp_size * kv_rows
    own = tp_size * q_rows
    firsts = [-(-(c * own) // block) for c in range(columns)]
    early = max(min((c + 1) * own // block - firsts[c] for c in range(columns)), 0)
    q_blocks = columns * own // block
    first = (column * own + block - 1) // block
    left = q_blocks - early
    places = [jnp.where(side == 0, left - 1 - i, i) for i in range(left)]
    last = [jnp.where(i >= first, i + early, i) for i in places]
    alone = left > 1
    for c in range(columns):
        for s in range(2):
            i = 0 if s else left - 1
            low = (i + early if i >= firsts[c] else i) * block
            for part in range(low // (2 * q_rows), (low + block - 1) // (2 * q_rows) + 1):
                alone = alone and (part // 2 == c or part % 2 != s)
    here = [q_blocks, q_blocks + 1] + [first + i for i in range(early)]
    return here + last, len(here), int(alone)


def multiply(index, prompts, weights, result, at, block):
    tile = min(TILE, prompts.shape[0])
    rows = pl.ds(pl.multiple_of(index * block, block), block)
    cols = rows if at is None else pl.ds(at * block, block)

    @pl.loop(0, prompts.shape[0] // tile)
    def _(i):
        at_rows = pl.ds(pl.multiple_of(i * tile, tile), tile)
        result[at_rows, cols] = lax.dot_general(
            prompts[at_rows, :], weights[rows, :], (((1,), (1,)), ((), ())),
            preferred_element_type=jnp.float32,
        ).astype(result.dtype)


def finish_kernel(
    columns, tp_size, q_rows, kv_rows,
    weights, prompts, partial, combined, projected, result, weight_sem, partial_sem, result_sem,
):
    r, t = lax.axis_index("rep"), lax.axis_index("tp")
    block = columns * tp_size * kv_rows
    blocks, soon, late_block = order_of(columns, tp_size, q_rows, kv_rows, r % columns, t // 2)
    done = soon + late_block
    stores = []
    for i in range(weights.shape[0] // block):
        at = pl.ds(i * block, block)
        stores.append(pltpu.make_async_copy(weights.at[at], combined.at[at], weight_sem.at[i]))
    for i in range(done):
        at = pl.ds(pl.multiple_of(blocks[i] * block, block), block)
        stores.append(pltpu.make_async_copy(partial.at[:, at], projected.at[:, at], partial_sem.at[i]))
    for store in stores:
        store.start()
    for i in range(done, len(blocks)):
        multiply(blocks[i], prompts, weights, result, i - done, block)
        at = pl.ds(pl.multiple_of(blocks[i] * block, block), block)
        store = pltpu.make_async_copy(result.at[:, pl.ds((i - done) * block, block)], projected.at[:, at], result_sem.at[i - done])
        store.start()
        stores.append(store)
    for store in stores:
        store.wait()


def gather_kernel(
    rep_size, tp_size, q_rows, kv_rows, piece, twice,
    q_weight, k_weight, v_weight, tok, weights, prompts, projected,
    relay, shard, wide, load_sem, local_sem,
    part_send, part_recv, z_send, z_recv, y_send, y_recv, x_send, x_recv, tok_send, tok_recv,
    pair_recv, twin_send, twin_recv,
):
    planes = tp_size
    columns = rep_size // planes
    half = tp_size // 2
    r, t = lax.axis_index("rep"), lax.axis_index("tp")
    plane, column = r // columns, r % columns
    side, core = t // 2, t % 2
    other = (t + half) % tp_size
    partner = t + 1 - 2 * core
    split = kv_rows // piece
    q_pieces = q_rows // piece
    pieces = q_pieces + 2 * split
    count = 2 * pieces
    small = 4 * split
    shards_in_plane = tp_size * columns
    ranks = (t, other)
    sequence = [(True, m) for m in range(2 * split)] + [(False, m) for m in range(2 * split)]
    for m in range(2 * split, pieces):
        sequence += [(True, m), (False, m)]

    def shard_row(m):
        return q_rows + m * piece if m < 2 * split else (m - 2 * split) * piece

    def row_of(index, m):
        if m >= 2 * split:
            return pl.multiple_of(index * q_rows + (m - 2 * split) * piece, 8)
        base = shards_in_plane * (q_rows + (m // split) * kv_rows) + (m % split) * piece
        return pl.multiple_of(base + index * kv_rows, 8)

    def in_weights(at_column, at_side, n):
        own, m = sequence[n]
        of_core = core if own else 1 - core
        return weights.at[pl.ds(row_of(at_column * tp_size + at_side * 2 + of_core, m), piece)]

    def in_relay(n):
        return relay.at[pl.ds(n * piece, piece)]

    def in_shard(m):
        return shard.at[pl.ds(shard_row(m), piece)]

    def place(slot, n):
        return in_weights(column, side, n) if slot == 0 else in_relay(n)

    def twin_place(d, n):
        return in_weights((column - d) % columns, side, n)

    def remote(src, dst, send, recv, to_rep, to_tp):
        return pltpu.make_async_remote_copy(
            src_ref=src, dst_ref=dst, send_sem=send, recv_sem=recv,
            device_id=(to_rep, to_tp), device_id_type=MESH,
        )

    def inner(k):
        return (k > 0) & (k < planes - 1)

    def reached(k, at):
        return (at != k) & (inner(k) | (at == k + 1) | (at == k - 1))

    def is_twice(n):
        return n >= count - twice

    def ups(slot):
        k = ranks[slot]
        return (plane >= k) & (plane < planes - 1), (plane <= k) & (plane > 0)

    def held_back(slot):
        k = ranks[slot]
        return (plane == k) & (k == planes - 2), (plane == k) & (k == 1)

    def late_sink(slot):
        k = ranks[slot]
        return ((plane == planes - 1) & (k == planes - 2)) | ((plane == 0) & (k == 1))

    def x_sends(n, src, dst, sem_of):
        for d in range(1, columns):
            to = plane * columns + (column + d) % columns
            remote(src, dst, x_send.at[d - 1], sem_of(d - 1), to, t).start()

    def forward(slot, n, src, source=False):
        up, down = ups(slot)
        if source:
            late_up, late_down = held_back(slot)
            up, down = up & jnp.logical_not(late_up), down & jnp.logical_not(late_down)
        dst = place(slot, n)

        @pl.when(up)
        def _():
            remote(src, dst, z_send.at[slot, 0], z_recv.at[slot, n], r + columns, t).start()

        @pl.when(down)
        def _():
            remote(src, dst, z_send.at[slot, 1], z_recv.at[slot, n], r - columns, t).start()

        if slot == 1:
            remote(src, in_weights(column, side, n), y_send.at[0], y_recv.at[n], r, other).start()
        elif not is_twice(n):
            x_sends(n, src, dst, lambda d: x_recv.at[d, 0 if n < small else 1])
        elif source:
            x_sends(n, src, dst, lambda d: pair_recv.at[d, n - (count - twice)])
        else:
            @pl.when(jnp.logical_not(reached(t, plane)))
            def _():
                x_sends(n, src, dst, lambda d: x_recv.at[d, 3])

    def span(n):
        return weights.at[pl.ds(0, n * piece)]

    def recv_wait(dst, sem):
        remote(dst, dst, x_send.at[0], sem, r, partner).wait_recv()

    def send_wait(src, sem):
        remote(src, src, sem, x_recv.at[0, 0], r, partner).wait_send()

    def at_source(slot, n):
        own, m = sequence[n]
        return in_shard(m) if own else place(slot, n)

    taken = [0, 0]

    def take(slot, n):
        while taken[slot] <= n:
            own, m = sequence[taken[slot]]
            if not own:
                @pl.when(plane == ranks[slot])
                def _():
                    recv_wait(place(slot, taken[slot]), part_recv.at[m])
            taken[slot] += 1

    def source_step(slot, n):
        take(slot, n)

        @pl.when(plane == ranks[slot])
        def _():
            forward(slot, n, at_source(slot, n), True)

    def late_step(slot, n):
        take(slot, n)
        late_up, late_down = held_back(slot)
        src, dst = at_source(slot, n), place(slot, n)

        @pl.when(late_up)
        def _():
            remote(src, dst, z_send.at[slot, 0], z_recv.at[slot, n], r + columns, t).start()

        @pl.when(late_down)
        def _():
            remote(src, dst, z_send.at[slot, 1], z_recv.at[slot, n], r - columns, t).start()

    def relay_step(slot, n, late):
        sink = late_sink(slot)

        @pl.when((plane != ranks[slot]) & (sink if late else jnp.logical_not(sink)))
        def _():
            recv_wait(place(slot, n), z_recv.at[slot, n])
            forward(slot, n, place(slot, n))

    def y_step(n, late):
        sink = late_sink(0)

        @pl.when(sink if late else jnp.logical_not(sink))
        def _():
            block = in_weights(column, 1 - side, n)
            recv_wait(block, y_recv.at[n])
            x_sends(n, block, block, lambda d: x_recv.at[d, 0 if n < small else 2])

    goes_up = (plane >= t) & (plane < planes - 1) & reached(t, plane + 1)
    goes_down = (plane <= t) & (plane > 0) & reached(t, plane - 1)
    goes = goes_up | goes_down

    def twin_step(d, n, source):
        src = twin_place(d, n)
        at = n - (count - twice)
        here = plane == t if source else (plane != t) & goes

        @pl.when(here)
        def _():
            recv_wait(src, pair_recv.at[d - 1, at] if source else twin_recv.at[d - 1, at])

        @pl.when(here & goes_up)
        def _():
            remote(src, src, twin_send.at[0], twin_recv.at[d - 1, at], r + columns, t).start()

        @pl.when(here & goes_down)
        def _():
            remote(src, src, twin_send.at[1], twin_recv.at[d - 1, at], r - columns, t).start()

    def twin_sink(d, n):
        @pl.when(reached(t, plane) & jnp.logical_not(goes))
        def _():
            recv_wait(twin_place(d, n), twin_recv.at[d - 1, n - (count - twice)])

    handler = core == plane % 2
    rows = tok.shape[0]
    chunk = rows // TOK_CHUNKS

    def prompt_rows(rank):
        return prompts.at[pl.ds(pl.multiple_of(rank * rows, 8), rows)]

    def prompt_chunk(rank, i):
        return prompts.at[pl.ds(pl.multiple_of(rank * rows + i * chunk, 8), chunk)]

    barrier = pltpu.get_barrier_semaphore()

    def greet(to_rep, to_tp):
        pl.semaphore_signal(barrier, inc=1, device_id=(to_rep, to_tp), device_id_type=MESH)

    @pl.when(plane < planes - 1)
    def _():
        greet(r + columns, t)

    @pl.when(plane > 0)
    def _():
        greet(r - columns, t)

    for d in range(1, columns):
        greet(plane * columns + (column + d) % columns, t)
    greet(r, other)
    greet(r, partner)

    loads = [
        pltpu.make_async_copy(k_weight, wide.at[pl.ds(q_rows, kv_rows)], load_sem.at[0]),
        pltpu.make_async_copy(v_weight, wide.at[pl.ds(q_rows + kv_rows, kv_rows)], load_sem.at[1]),
        pltpu.make_async_copy(q_weight, wide.at[pl.ds(0, q_rows)], load_sem.at[2]),
    ]
    load_tok = pltpu.make_async_copy(tok, prompt_rows(t), local_sem.at[0])
    for load in loads:
        load.start()
    load_tok.start()

    def cast(m):
        at = pl.ds(shard_row(m), piece)
        value = wide[at, :].astype(shard.dtype)
        shard[at, :] = value

        @pl.when(plane == t)
        def _():
            weights[pl.ds(row_of(column * tp_size + t, m), piece), :] = value

    def part(m):
        @pl.when(jnp.logical_not(handler))
        def _():
            @pl.when(side == plane // 2)
            def _():
                dst = weights.at[pl.ds(row_of(column * tp_size + t, m), piece)]
                remote(in_shard(m), dst, part_send.at[0], part_recv.at[m], r, partner).start()

            @pl.when(side != plane // 2)
            def _():
                remote(in_shard(m), in_relay(sequence.index((False, m))), part_send.at[0], part_recv.at[m], r, partner).start()

    loads[0].wait()
    loads[1].wait()
    for m in range(2 * split):
        cast(m)
    neighbours = columns + 1 + jnp.where(inner(plane), 2, 1)
    pl.semaphore_wait(barrier, neighbours)
    for m in range(2 * split):
        part(m)
    lead = min(LEAD, 2 * split)
    for n in range(lead):
        source_step(0, n)
        source_step(1, n)
    loads[2].wait()
    for m in range(2 * split, pieces):
        cast(m)
    for m in range(2 * split, pieces):
        part(m)
    for n in range(lead, LEAD):
        source_step(0, n)
        source_step(1, n)
    load_tok.wait()
    remote(tok, prompt_rows(t), tok_send.at[1], tok_recv.at[1], r, partner).start()

    late, sunk, late_y, sent, twins, far = [0, 0], [0, 0], 0, 0, 0, 0
    pairs = [(d, n) for n in range(count - twice, count) for d in range(1, columns)]
    block = shards_in_plane * kv_rows
    blocks, soon, late_block = order_of(columns, tp_size, q_rows, kv_rows, column, side)

    def late_to(slot, stop):
        while late[slot] < min(stop, count):
            late_step(slot, late[slot])
            late[slot] += 1

    def sink_to(slot, stop):
        while sunk[slot] < min(stop, count):
            relay_step(slot, sunk[slot], True)
            sunk[slot] += 1

    def late_y_to(stop):
        nonlocal late_y
        while late_y < min(stop, count):
            y_step(late_y, True)
            late_y += 1

    def send_tokens(stop):
        nonlocal sent
        while sent < min(stop, TOK_CHUNKS):
            at = pl.ds(sent * chunk, chunk)
            remote(tok.at[at], prompt_chunk(t, sent), tok_send.at[0], tok_recv.at[0], r, other).start()
            sent += 1

    def twins_to(stop):
        nonlocal twins
        while twins < min(stop, len(pairs)):
            twin_step(*pairs[twins], True)
            twins += 1

    def far_to(stop):
        nonlocal far
        while far < min(stop, len(pairs)):
            twin_step(*pairs[far], False)
            far += 1

    def meet():
        recv_wait(prompt_rows(other), tok_recv.at[0])
        remote(prompt_rows(other), prompt_rows(other), tok_send.at[2], tok_recv.at[2], r, partner).start()

    def begin():
        recv_wait(prompt_rows(partner), tok_recv.at[1])
        recv_wait(prompt_rows((partner + half) % tp_size), tok_recv.at[2])
        for d in range(1, columns):
            recv_wait(span(2 * small), x_recv.at[d - 1, 0])

    send_tokens(TOK_FIRST)
    for slot in range(2):
        late_to(slot, LATE_FIRST[slot])
    for n in range(count):
        for slot in range(2):
            late_to(slot, LATE_FIRST[slot] + (n + 1) * LATE_RATE[slot] // 4)
        if n + LEAD < count:
            source_step(0, n + LEAD)
            source_step(1, n + LEAD)
        relay_step(0, n, False)
        relay_step(1, n, False)
        for slot in range(2):
            sink_to(slot, (n + 1) * LATE_RATE[slot] // 4)
        if n >= TOK_AT:
            send_tokens(TOK_FIRST + (n - TOK_AT) * TOK_RATE // 4 + 1)
        if n >= Y_LAG:
            y_step(n - Y_LAG, False)
        late_y_to((n + 1) * min(LATE_RATE) // 4 - Y_LAG)
        if twice and n >= TWIN_AT:
            twins_to((n - TWIN_AT) * TWIN_RATE // 4 + 1)
        if twice and n >= FAR_AT:
            far_to((n - FAR_AT) * TWIN_RATE // 4 + 1)
        if n == MEET_AT:
            meet()
        for i in range(2):
            if n == FIRST_AT[i]:
                if i == 0:
                    begin()
                multiply(blocks[i], prompts, weights, projected, None, block)
    for slot in range(2):
        late_to(slot, count)
    for n in range(count - Y_LAG, count):
        y_step(n, False)
    early = [i for i in range(2) if FIRST_AT[i] < count]
    if MEET_AT >= count:
        meet()
    if not early:
        begin()
    rest = [i for i in range(soon) if i not in early]
    twins_to(len(pairs))
    before = [i for i in rest if i < 2]
    after = [i for i in rest if i >= 2]
    steps = max(count - min(sunk), 1)
    for k in range(steps):
        for slot in range(2):
            sink_to(slot, max(sunk[slot], min(sunk) + 1) if k < steps - 1 else count)
        late_y_to(min(sunk) - Y_LAG)
        far_to(len(pairs) * (k + 1) // steps)
        if before and (k + 1) % max(steps // (len(before) + 1), 1) == 0:
            multiply(blocks[before.pop(0)], prompts, weights, projected, None, block)
    late_y_to(count)
    far_to(len(pairs))
    for i in before + after:
        multiply(blocks[i], prompts, weights, projected, None, block)
    for d in range(1, columns):
        recv_wait(span(count - small), x_recv.at[d - 1, 2])
    if late_block:
        multiply(blocks[soon], prompts, weights, projected, None, block)
    for d, n in pairs:
        twin_sink(d, n)
    for d in range(1, columns):
        recv_wait(span(count - twice - small), x_recv.at[d - 1, 1])
        if twice:
            @pl.when((plane != t) & jnp.logical_not(reached(t, plane)))
            def _():
                recv_wait(span(twice), x_recv.at[d - 1, 3])

    for d in range(1, columns):
        send_wait(span(2 * count - twice), x_send.at[d - 1])
        if twice:
            @pl.when(jnp.logical_not(reached(t, plane)))
            def _():
                send_wait(span(twice), x_send.at[d - 1])
    send_wait(relay, y_send.at[0])
    for slot in range(2):
        for way, go in enumerate(ups(slot)):
            @pl.when(go)
            def _():
                send_wait(relay, z_send.at[slot, way])
    if twice:
        @pl.when(goes_up)
        def _():
            send_wait(span(twice * (columns - 1)), twin_send.at[0])

        @pl.when(goes_down)
        def _():
            send_wait(span(twice * (columns - 1)), twin_send.at[1])

    @pl.when(jnp.logical_not(handler))
    def _():
        send_wait(shard, part_send.at[0])

    for i in range(3):
        send_wait(tok, tok_send.at[i])


def shards(q_weight, key_projection_weight, value_projection_weight, tokens):
    rep_size, tp_size = lax.axis_size("rep"), lax.axis_size("tp")
    columns = rep_size // tp_size
    q_rows, width = q_weight.shape
    kv_rows = key_projection_weight.shape[0]
    piece = kv_rows // 2 if kv_rows % 32 == 0 else kv_rows
    pieces = (q_rows + 2 * kv_rows) // piece
    count = 2 * pieces
    twice = count * TWICE[0] // TWICE[1] if columns == 2 else 0
    hbm = pl.BlockSpec(memory_space=pltpu.HBM)
    dma = pltpu.SemaphoreType.DMA
    dtype = tokens.dtype
    block = columns * tp_size * kv_rows
    rows = tp_size * tokens.shape[0]
    each = q_rows + 2 * kv_rows
    total = columns * tp_size * each
    vmem = pl.BlockSpec(memory_space=pltpu.VMEM)
    inputs = [
        pltpu.with_memory_space_constraint(a, pltpu.HBM)
        for a in (q_weight, key_projection_weight, value_projection_weight, tokens)
    ]
    held = pl.pallas_call(
        functools.partial(gather_kernel, rep_size, tp_size, q_rows, kv_rows, piece, twice),
        out_shape=(
            pltpu.VMEM((total, width), dtype),
            pltpu.VMEM((rows, width), dtype),
            pltpu.VMEM((rows, total), dtype),
        ),
        in_specs=[hbm] * 4,
        out_specs=(vmem,) * 3,
        scratch_shapes=[
            pltpu.VMEM((count * piece, width), dtype),
            pltpu.VMEM((each, width), dtype),
            pltpu.VMEM((each, width), q_weight.dtype),
            dma((3,)), dma((1,)),
            dma((1,)), dma((pieces,)),
            dma((2, 2)), dma((2, count)),
            dma((1,)), dma((count,)),
            dma((columns - 1,)), dma((columns - 1, 4)),
            dma((3,)), dma((3,)),
            dma((columns - 1, max(twice, 1))), dma((2,)), dma((columns - 1, max(twice, 1))),
        ],
        compiler_params=pltpu.CompilerParams(
            has_side_effects=True, collective_id=0, vmem_limit_bytes=VMEM * 2**20
        ),
    )(*inputs)
    blocks = total // block
    return pl.pallas_call(
        functools.partial(finish_kernel, columns, tp_size, q_rows, kv_rows),
        out_shape=(
            jax.ShapeDtypeStruct((total, width), dtype),
            jax.ShapeDtypeStruct((rows, total), dtype),
        ),
        in_specs=[vmem] * 3,
        out_specs=(hbm, hbm),
        scratch_shapes=[
            pltpu.VMEM((rows, total), dtype), dma((blocks,)), dma((blocks,)), dma((blocks,)),
        ],
        compiler_params=pltpu.CompilerParams(vmem_limit_bytes=VMEM * 2**20),
    )(*held)


def solution(mesh):
    spec = P(("rep", "tp"), None)
    return jax.shard_map(
        shards, mesh=mesh, in_specs=(spec,) * 4, out_specs=(P("tp", None), P("rep", "tp")), check_vma=False
    )
```

```python
import functools

import jax
import jax.numpy as jnp
from jax import lax
from jax.experimental import pallas as pl
from jax.experimental.pallas import tpu as pltpu
from jax.sharding import PartitionSpec as P

MESH = pl.DeviceIdType.MESH
LEAD = 4
Y_LAG = 3
LATE_FIRST = (1, 2)
LATE_RATE = (6, 5)
TOK_FIRST = 2
TOK_AT = 8
TOK_RATE = 2
TOK_CHUNKS = 8
TWIN_AT = 18
TWIN_RATE = 4
FAR_AT = 24
MEET_AT = 22
BLOCK_AT = (6, 12)
TWICE = (17, 28)
NEAR = (14, 28)
CROSS = 1
TILE = 512
VMEM = 20


def order_of(columns, tp_size, q_rows, kv_rows, column):
    block = columns * tp_size * kv_rows
    own = tp_size * q_rows
    firsts = [-(-(c * own) // block) for c in range(columns)]
    early = max(min((c + 1) * own // block - firsts[c] for c in range(columns)), 0)
    q_blocks = columns * own // block
    first = (column * own + block - 1) // block
    rest = [jnp.where(i >= first, i + early, i) for i in range(q_blocks - early)]
    return [first + i for i in range(early)] + rest + [q_blocks, q_blocks + 1], early


def multiply(index, prompts, weights, result, at, block):
    tile = min(TILE, prompts.shape[0])
    rows = pl.ds(pl.multiple_of(index * block, block), block)
    cols = rows if at is None else pl.ds(at * block, block)

    @pl.loop(0, prompts.shape[0] // tile)
    def _(i):
        at_rows = pl.ds(pl.multiple_of(i * tile, tile), tile)
        result[at_rows, cols] = lax.dot_general(
            prompts[at_rows, :], weights[rows, :], (((1,), (1,)), ((), ())),
            preferred_element_type=jnp.float32,
        ).astype(result.dtype)


def finish_kernel(
    columns, tp_size, q_rows, kv_rows,
    weights, prompts, partial, combined, projected, result, weight_sem, partial_sem, result_sem,
):
    r, t = lax.axis_index("rep"), lax.axis_index("tp")
    block = columns * tp_size * kv_rows
    blocks, _ = order_of(columns, tp_size, q_rows, kv_rows, r % columns)
    done = len(blocks) - 2
    stores = []
    for i in range(weights.shape[0] // block):
        at = pl.ds(i * block, block)
        stores.append(pltpu.make_async_copy(weights.at[at], combined.at[at], weight_sem.at[i]))
    for i in range(done):
        at = pl.ds(pl.multiple_of(blocks[i] * block, block), block)
        stores.append(pltpu.make_async_copy(partial.at[:, at], projected.at[:, at], partial_sem.at[i]))
    for store in stores:
        store.start()
    for i in range(done, len(blocks)):
        multiply(blocks[i], prompts, weights, result, i - done, block)
        at = pl.ds(pl.multiple_of(blocks[i] * block, block), block)
        store = pltpu.make_async_copy(result.at[:, pl.ds((i - done) * block, block)], projected.at[:, at], result_sem.at[i - done])
        store.start()
        stores.append(store)
    for store in stores:
        store.wait()


def gather_kernel(
    rep_size, tp_size, q_rows, kv_rows, piece, twice, near,
    q_weight, k_weight, v_weight, tok, weights, prompts, projected,
    relay, shard, wide, load_sem, local_sem,
    part_send, part_recv, z_send, z_recv, y_send, y_recv, x_send, x_recv, tok_send, tok_recv,
    pair_recv, twin_send, twin_recv, cross_send, cross_recv,
):
    planes = tp_size
    columns = rep_size // planes
    half = tp_size // 2
    r, t = lax.axis_index("rep"), lax.axis_index("tp")
    plane, column = r // columns, r % columns
    side, core = t // 2, t % 2
    other = (t + half) % tp_size
    partner = t + 1 - 2 * core
    split = kv_rows // piece
    q_pieces = q_rows // piece
    pieces = q_pieces + 2 * split
    count = 2 * pieces
    large = 2 * q_pieces
    shards_in_plane = tp_size * columns
    ranks = (t, other)

    def sequence(n):
        return n % 2 == 0, n // 2

    def row_of(index, m):
        if m < q_pieces:
            return pl.multiple_of(index * q_rows + m * piece, 8)
        m -= q_pieces
        base = shards_in_plane * (q_rows + (m // split) * kv_rows) + (m % split) * piece
        return pl.multiple_of(base + index * kv_rows, 8)

    def in_weights(at_column, at_side, n):
        own, m = sequence(n)
        of_core = core if own else 1 - core
        return weights.at[pl.ds(row_of(at_column * tp_size + at_side * 2 + of_core, m), piece)]

    def in_relay(n):
        return relay.at[pl.ds(n * piece, piece)]

    def in_shard(m):
        return shard.at[pl.ds(m * piece, piece)]

    def place(slot, n):
        return in_weights(column, side, n) if slot == 0 else in_relay(n)

    def twin_place(d, n):
        return in_weights((column - d) % columns, side, n)

    def remote(src, dst, send, recv, to_rep, to_tp):
        return pltpu.make_async_remote_copy(
            src_ref=src, dst_ref=dst, send_sem=send, recv_sem=recv,
            device_id=(to_rep, to_tp), device_id_type=MESH,
        )

    def inner(k):
        return (k > 0) & (k < planes - 1)

    def reached(k, at):
        return (at != k) & (inner(k) | (at == k + 1) | (at == k - 1))

    def beside(k, at):
        return ((k == 1) & (at == 0)) | ((k == planes - 2) & (at == planes - 1))

    def doubled(n, at):
        if n >= count - near:
            return reached(t, at)
        return reached(t, at) & jnp.logical_not(beside(t, at))

    def is_twice(n):
        return n >= count - twice

    def ups(slot):
        k = ranks[slot]
        return (plane >= k) & (plane < planes - 1), (plane <= k) & (plane > 0)

    def held_back(slot):
        k = ranks[slot]
        return (plane == k) & (k == planes - 2), (plane == k) & (k == 1)

    def late_sink(slot):
        k = ranks[slot]
        return ((plane == planes - 1) & (k == planes - 2)) | ((plane == 0) & (k == 1))

    def x_sends(n, src, dst, sem_of):
        for d in range(1, columns):
            to = plane * columns + (column + d) % columns
            remote(src, dst, x_send.at[d - 1], sem_of(d - 1), to, t).start()

    def forward(slot, n, src, source=False):
        up, down = ups(slot)
        if source:
            late_up, late_down = held_back(slot)
            up, down = up & jnp.logical_not(late_up), down & jnp.logical_not(late_down)
        dst = place(slot, n)

        @pl.when(up)
        def _():
            remote(src, dst, z_send.at[slot, 0], z_recv.at[slot, n], r + columns, t).start()

        @pl.when(down)
        def _():
            remote(src, dst, z_send.at[slot, 1], z_recv.at[slot, n], r - columns, t).start()

        if slot == 1:
            remote(src, in_weights(column, side, n), y_send.at[0], y_recv.at[n], r, other).start()
        elif not is_twice(n):
            x_sends(n, src, dst, lambda d: x_recv.at[d, 1 if n < large else 0])
        elif source:
            x_sends(n, src, dst, lambda d: pair_recv.at[d, n - (count - twice)])
        else:
            @pl.when(jnp.logical_not(doubled(n, plane)))
            def _():
                x_sends(n, src, dst, lambda d: x_recv.at[d, 3 if n < large else 4])

    def span(n):
        return weights.at[pl.ds(0, n * piece)]

    def recv_wait(dst, sem):
        remote(dst, dst, x_send.at[0], sem, r, partner).wait_recv()

    def send_wait(src, sem):
        remote(src, src, sem, x_recv.at[0, 0], r, partner).wait_send()

    def at_source(slot, n):
        own, m = sequence(n)
        return in_shard(m) if own else place(slot, n)

    taken = [0, 0]

    def take(slot, n):
        while taken[slot] <= n:
            own, m = sequence(taken[slot])
            if not own:
                @pl.when(plane == ranks[slot])
                def _():
                    recv_wait(place(slot, taken[slot]), part_recv.at[m])
            taken[slot] += 1

    def source_step(slot, n):
        take(slot, n)

        @pl.when(plane == ranks[slot])
        def _():
            forward(slot, n, at_source(slot, n), True)

    def late_step(slot, n):
        take(slot, n)
        if slot == 1 and n < CROSS:
            return
        late_up, late_down = held_back(slot)
        src, dst = at_source(slot, n), place(slot, n)

        @pl.when(late_up)
        def _():
            remote(src, dst, z_send.at[slot, 0], z_recv.at[slot, n], r + columns, t).start()

        @pl.when(late_down)
        def _():
            remote(src, dst, z_send.at[slot, 1], z_recv.at[slot, n], r - columns, t).start()

    def relay_step(slot, n, late):
        sink = late_sink(slot)
        if slot == 1 and late and n < CROSS:
            return

        @pl.when((plane != ranks[slot]) & (sink if late else jnp.logical_not(sink)))
        def _():
            recv_wait(place(slot, n), z_recv.at[slot, n])
            forward(slot, n, place(slot, n))

    def y_step(n, late):
        sink = late_sink(0)

        @pl.when(sink if late else jnp.logical_not(sink))
        def _():
            block = in_weights(column, 1 - side, n)
            recv_wait(block, cross_recv.at[n] if late and n < CROSS else y_recv.at[n])
            x_sends(n, block, block, lambda d: x_recv.at[d, 2 if n < large else 0])
            if n < CROSS and not late:
                @pl.when((plane == t) & (t == 1))
                def _():
                    remote(block, block, cross_send.at[0], cross_recv.at[n], r - columns, t).start()

                @pl.when((plane == t) & (t == planes - 2))
                def _():
                    remote(block, block, cross_send.at[0], cross_recv.at[n], r + columns, t).start()

    def goes_up(n):
        return (plane >= t) & (plane < planes - 1) & doubled(n, plane + 1)

    def goes_down(n):
        return (plane <= t) & (plane > 0) & doubled(n, plane - 1)

    def goes(n):
        return goes_up(n) | goes_down(n)

    def twin_step(d, n, source):
        src = twin_place(d, n)
        at = n - (count - twice)
        here = plane == t if source else (plane != t) & goes(n)

        @pl.when(here)
        def _():
            recv_wait(src, pair_recv.at[d - 1, at] if source else twin_recv.at[d - 1, at])

        @pl.when(here & goes_up(n))
        def _():
            remote(src, src, twin_send.at[0], twin_recv.at[d - 1, at], r + columns, t).start()

        @pl.when(here & goes_down(n))
        def _():
            remote(src, src, twin_send.at[1], twin_recv.at[d - 1, at], r - columns, t).start()

    def twin_sink(d, n):
        @pl.when(doubled(n, plane) & jnp.logical_not(goes(n)))
        def _():
            recv_wait(twin_place(d, n), twin_recv.at[d - 1, n - (count - twice)])

    handler = core == plane % 2
    rows = tok.shape[0]
    chunk = rows // TOK_CHUNKS

    def prompt_rows(rank):
        return prompts.at[pl.ds(pl.multiple_of(rank * rows, 8), rows)]

    def prompt_chunk(rank, i):
        return prompts.at[pl.ds(pl.multiple_of(rank * rows + i * chunk, 8), chunk)]

    barrier = pltpu.get_barrier_semaphore()

    def greet(to_rep, to_tp):
        pl.semaphore_signal(barrier, inc=1, device_id=(to_rep, to_tp), device_id_type=MESH)

    @pl.when(plane < planes - 1)
    def _():
        greet(r + columns, t)

    @pl.when(plane > 0)
    def _():
        greet(r - columns, t)

    for d in range(1, columns):
        greet(plane * columns + (column + d) % columns, t)
    greet(r, other)
    greet(r, partner)

    chunks = q_rows // kv_rows
    loads = [
        pltpu.make_async_copy(
            q_weight.at[pl.ds(i * kv_rows, kv_rows)], wide.at[pl.ds(i * kv_rows, kv_rows)], load_sem.at[i]
        )
        for i in range(chunks)
    ] + [
        pltpu.make_async_copy(w, wide.at[pl.ds(q_rows + i * kv_rows, kv_rows)], load_sem.at[chunks + i])
        for i, w in enumerate((k_weight, v_weight))
    ]
    load_tok = pltpu.make_async_copy(tok, prompt_rows(t), local_sem.at[0])
    for load in loads:
        load.start()
    load_tok.start()

    def cast(m):
        at = pl.ds(m * piece, piece)
        value = wide[at, :].astype(shard.dtype)
        shard[at, :] = value

        @pl.when(plane == t)
        def _():
            weights[pl.ds(row_of(column * tp_size + t, m), piece), :] = value

    def part(m):
        @pl.when(jnp.logical_not(handler))
        def _():
            @pl.when(side == plane // 2)
            def _():
                dst = weights.at[pl.ds(row_of(column * tp_size + t, m), piece)]
                remote(in_shard(m), dst, part_send.at[0], part_recv.at[m], r, partner).start()

            @pl.when(side != plane // 2)
            def _():
                remote(in_shard(m), in_relay(2 * m + 1), part_send.at[0], part_recv.at[m], r, partner).start()

    loads[0].wait()
    for m in range(split):
        cast(m)
    neighbours = columns + 1 + jnp.where(inner(plane), 2, 1)
    pl.semaphore_wait(barrier, neighbours)
    for m in range(split):
        part(m)
    lead = min(LEAD, 2 * split)
    for n in range(lead):
        source_step(0, n)
        source_step(1, n)
    for i in range(1, chunks + 2):
        loads[i].wait()
        for m in range(i * split, (i + 1) * split):
            cast(m)
            part(m)
    for n in range(lead, LEAD):
        source_step(0, n)
        source_step(1, n)
    load_tok.wait()
    remote(tok, prompt_rows(t), tok_send.at[1], tok_recv.at[1], r, partner).start()

    late, sunk, late_y, sent, twins, far = [0, 0], [0, 0], 0, 0, 0, 0
    pairs = [(d, n) for n in range(count - twice, count) for d in range(1, columns)]
    block = shards_in_plane * kv_rows
    blocks, own_blocks = order_of(columns, tp_size, q_rows, kv_rows, column)

    def late_to(slot, stop):
        while late[slot] < min(stop, count):
            late_step(slot, late[slot])
            late[slot] += 1

    def sink_to(slot, stop):
        while sunk[slot] < min(stop, count):
            relay_step(slot, sunk[slot], True)
            sunk[slot] += 1

    def late_y_to(stop):
        nonlocal late_y
        while late_y < min(stop, count):
            y_step(late_y, True)
            late_y += 1

    def send_tokens(stop):
        nonlocal sent
        while sent < min(stop, TOK_CHUNKS):
            at = pl.ds(sent * chunk, chunk)
            remote(tok.at[at], prompt_chunk(t, sent), tok_send.at[0], tok_recv.at[0], r, other).start()
            sent += 1

    def twins_to(stop):
        nonlocal twins
        while twins < min(stop, len(pairs)):
            twin_step(*pairs[twins], True)
            twins += 1

    def far_to(stop):
        nonlocal far
        while far < min(stop, len(pairs)):
            twin_step(*pairs[far], False)
            far += 1

    def meet():
        recv_wait(prompt_rows(other), tok_recv.at[0])
        remote(prompt_rows(other), prompt_rows(other), tok_send.at[2], tok_recv.at[2], r, partner).start()

    def begin():
        recv_wait(prompt_rows(partner), tok_recv.at[1])
        recv_wait(prompt_rows((partner + half) % tp_size), tok_recv.at[2])

    def arrive(first, stop, sems):
        plain = max(min(stop, count - twice) - first, 0)
        extra = stop - first - plain
        for d in range(1, columns):
            if sems[0] != sems[1]:
                if plain:
                    recv_wait(span(plain), x_recv.at[d - 1, sems[0]])
                recv_wait(span(stop - first), x_recv.at[d - 1, sems[1]])
            else:
                recv_wait(span(plain + stop - first), x_recv.at[d - 1, sems[0]])
            if extra:
                @pl.when((plane != t) & jnp.logical_not(reached(t, plane)))
                def _():
                    recv_wait(span(extra), x_recv.at[d - 1, sems[2]])
            single = max(min(stop, count - near) - max(first, count - twice), 0)
            if single:
                @pl.when(beside(t, plane))
                def _():
                    recv_wait(span(single), x_recv.at[d - 1, sems[2]])
        for d, n in pairs:
            if first <= n < stop:
                twin_sink(d, n)

    send_tokens(TOK_FIRST)
    for slot in range(2):
        late_to(slot, LATE_FIRST[slot])
    for n in range(count):
        for slot in range(2):
            late_to(slot, LATE_FIRST[slot] + (n + 1) * LATE_RATE[slot] // 4)
        if n + LEAD < count:
            source_step(0, n + LEAD)
            source_step(1, n + LEAD)
        relay_step(0, n, False)
        relay_step(1, n, False)
        for slot in range(2):
            sink_to(slot, (n + 1) * LATE_RATE[slot] // 4)
        if n >= TOK_AT:
            send_tokens(TOK_FIRST + (n - TOK_AT) * TOK_RATE // 4 + 1)
        if n >= Y_LAG:
            y_step(n - Y_LAG, False)
        late_y_to((n + 1) * min(LATE_RATE) // 4 - Y_LAG)
        if twice and n >= TWIN_AT:
            twins_to((n - TWIN_AT) * TWIN_RATE // 4 + 1)
        if twice and n >= FAR_AT:
            far_to((n - FAR_AT) * TWIN_RATE // 4 + 1)
        if n == MEET_AT:
            meet()
    for slot in range(2):
        late_to(slot, count)
    for n in range(count - Y_LAG, count):
        y_step(n, False)
    if MEET_AT >= count:
        meet()
    begin()
    twins_to(len(pairs))
    done = 0

    def multiply_to(stop):
        nonlocal done
        while done < stop:
            if done == own_blocks:
                arrive(0, large, (1, 2, 3))
            multiply(blocks[done], prompts, weights, projected, None, block)
            done += 1

    for slot in range(2):
        sink_to(slot, count)
    late_y_to(count)
    for i in range(len(pairs)):
        far_to(i + 1)
        multiply_to(sum(i >= at for at in BLOCK_AT[:own_blocks]))
    multiply_to(len(blocks) - 2)
    arrive(large, count, (0, 0, 4))

    def sent_when(go, n, sem):
        if n:
            @pl.when(go)
            def _():
                send_wait(span(n), sem)

    for d in range(1, columns):
        send_wait(span(2 * count - twice), x_send.at[d - 1])
        sent_when(jnp.logical_not(reached(t, plane)), twice, x_send.at[d - 1])
        sent_when(beside(t, plane), twice - near, x_send.at[d - 1])
    send_wait(span(count - CROSS), y_send.at[0])
    sent_when(jnp.logical_not(late_sink(1)), CROSS, y_send.at[0])
    for slot in range(2):
        for way in range(2):
            go, held = ups(slot)[way], held_back(slot)[way]
            sent_when(go, count - CROSS, z_send.at[slot, way])
            sent_when(go & jnp.logical_not(held) if slot else go, CROSS, z_send.at[slot, way])
    if twice:
        for way, go in enumerate((goes_up, goes_down)):
            sent_when(go(count - 1), near * (columns - 1), twin_send.at[way])
            sent_when(go(count - twice), (twice - near) * (columns - 1), twin_send.at[way])
    sent_when((plane == t) & inner(t), CROSS, cross_send.at[0])

    @pl.when(jnp.logical_not(handler))
    def _():
        send_wait(shard, part_send.at[0])

    for i in range(3):
        send_wait(tok, tok_send.at[i])


def shards(q_weight, key_projection_weight, value_projection_weight, tokens):
    rep_size, tp_size = lax.axis_size("rep"), lax.axis_size("tp")
    columns = rep_size // tp_size
    q_rows, width = q_weight.shape
    kv_rows = key_projection_weight.shape[0]
    piece = kv_rows // 2 if kv_rows % 32 == 0 else kv_rows
    pieces = (q_rows + 2 * kv_rows) // piece
    count = 2 * pieces
    twice, near = [count * a // b if columns == 2 else 0 for a, b in (TWICE, NEAR)]
    hbm = pl.BlockSpec(memory_space=pltpu.HBM)
    dma = pltpu.SemaphoreType.DMA
    dtype = tokens.dtype
    block = columns * tp_size * kv_rows
    rows = tp_size * tokens.shape[0]
    each = q_rows + 2 * kv_rows
    total = columns * tp_size * each
    vmem = pl.BlockSpec(memory_space=pltpu.VMEM)
    inputs = [
        pltpu.with_memory_space_constraint(a, pltpu.HBM)
        for a in (q_weight, key_projection_weight, value_projection_weight, tokens)
    ]
    held = pl.pallas_call(
        functools.partial(gather_kernel, rep_size, tp_size, q_rows, kv_rows, piece, twice, near),
        out_shape=(
            pltpu.VMEM((total, width), dtype),
            pltpu.VMEM((rows, width), dtype),
            pltpu.VMEM((rows, total), dtype),
        ),
        in_specs=[hbm] * 4,
        out_specs=(vmem,) * 3,
        scratch_shapes=[
            pltpu.VMEM((count * piece, width), dtype),
            pltpu.VMEM((each, width), dtype),
            pltpu.VMEM((each, width), q_weight.dtype),
            dma((q_rows // kv_rows + 2,)), dma((1,)),
            dma((1,)), dma((pieces,)),
            dma((2, 2)), dma((2, count)),
            dma((1,)), dma((count,)),
            dma((columns - 1,)), dma((columns - 1, 5)),
            dma((3,)), dma((3,)),
            dma((columns - 1, max(twice, 1))), dma((2,)), dma((columns - 1, max(twice, 1))),
            dma((1,)), dma((max(CROSS, 1),)),
        ],
        compiler_params=pltpu.CompilerParams(
            has_side_effects=True, collective_id=0, vmem_limit_bytes=VMEM * 2**20
        ),
    )(*inputs)
    blocks = total // block
    return pl.pallas_call(
        functools.partial(finish_kernel, columns, tp_size, q_rows, kv_rows),
        out_shape=(
            jax.ShapeDtypeStruct((total, width), dtype),
            jax.ShapeDtypeStruct((rows, total), dtype),
        ),
        in_specs=[vmem] * 3,
        out_specs=(hbm, hbm),
        scratch_shapes=[
            pltpu.VMEM((rows, 2 * block), dtype), dma((blocks,)), dma((blocks,)), dma((2,)),
        ],
        compiler_params=pltpu.CompilerParams(vmem_limit_bytes=VMEM * 2**20),
    )(*held)


def solution(mesh):
    spec = P(("rep", "tp"), None)
    return jax.shard_map(
        shards, mesh=mesh, in_specs=(spec,) * 4, out_specs=(P("tp", None), P("rep", "tp")), check_vma=False
    )
```

```python
import functools

import jax
import jax.numpy as jnp
from jax import lax
from jax.experimental import pallas as pl
from jax.experimental.pallas import tpu as pltpu
from jax.sharding import PartitionSpec as P

MESH = pl.DeviceIdType.MESH
LEAD = 4
Y_LAG = 3
LATE_FIRST = (1, 2)
LATE_RATE = (6, 5)
TOK_FIRST = 2
TOK_AT = 8
TOK_RATE = 2
TOK_CHUNKS = 8
TWIN_AT = 18
TWIN_RATE = 4
FAR_AT = 24
MEET_AT = 22
BLOCK_AT = (6, 12)
TWICE = (17, 28)
NEAR = (14, 28)
CROSS = 1
TILE = 512
VMEM = 20


def order_of(columns, tp_size, q_rows, kv_rows, column):
    block = columns * tp_size * kv_rows
    own = tp_size * q_rows
    firsts = [-(-(c * own) // block) for c in range(columns)]
    early = max(min((c + 1) * own // block - firsts[c] for c in range(columns)), 0)
    q_blocks = columns * own // block
    first = (column * own + block - 1) // block
    rest = [jnp.where(i >= first, i + early, i) for i in range(q_blocks - early)]
    return [first + i for i in range(early)] + rest + [q_blocks, q_blocks + 1], early


def multiply(index, prompts, weights, result, at, block):
    tile = min(TILE, prompts.shape[0])
    rows = pl.ds(pl.multiple_of(index * block, block), block)
    cols = rows if at is None else pl.ds(at * block, block)

    @pl.loop(0, prompts.shape[0] // tile)
    def _(i):
        at_rows = pl.ds(pl.multiple_of(i * tile, tile), tile)
        result[at_rows, cols] = lax.dot_general(
            prompts[at_rows, :], weights[rows, :], (((1,), (1,)), ((), ())),
            preferred_element_type=jnp.float32,
        ).astype(result.dtype)


def finish_kernel(
    columns, tp_size, q_rows, kv_rows,
    weights, prompts, partial, combined, projected, result, weight_sem, partial_sem, result_sem,
):
    r, t = lax.axis_index("rep"), lax.axis_index("tp")
    block = columns * tp_size * kv_rows
    blocks, _ = order_of(columns, tp_size, q_rows, kv_rows, r % columns)
    done = len(blocks) - 2
    stores = []
    for i in range(weights.shape[0] // block):
        at = pl.ds(i * block, block)
        stores.append(pltpu.make_async_copy(weights.at[at], combined.at[at], weight_sem.at[i]))
    for i in range(done):
        at = pl.ds(pl.multiple_of(blocks[i] * block, block), block)
        stores.append(pltpu.make_async_copy(partial.at[:, at], projected.at[:, at], partial_sem.at[i]))
    for store in stores:
        store.start()
    for i in range(done, len(blocks)):
        multiply(blocks[i], prompts, weights, result, i - done, block)
        at = pl.ds(pl.multiple_of(blocks[i] * block, block), block)
        store = pltpu.make_async_copy(result.at[:, pl.ds((i - done) * block, block)], projected.at[:, at], result_sem.at[i - done])
        store.start()
        stores.append(store)
    for store in stores:
        store.wait()


def gather_kernel(
    rep_size, tp_size, q_rows, kv_rows, piece, twice, near,
    q_weight, k_weight, v_weight, tok, weights, prompts, projected,
    relay, shard, wide, load_sem, local_sem,
    part_send, part_recv, z_send, z_recv, y_send, y_recv, x_send, x_recv, tok_send, tok_recv,
    pair_recv, twin_send, twin_recv, cross_send, cross_recv,
):
    planes = tp_size
    columns = rep_size // planes
    half = tp_size // 2
    r, t = lax.axis_index("rep"), lax.axis_index("tp")
    plane, column = r // columns, r % columns
    side, core = t // 2, t % 2
    other = (t + half) % tp_size
    partner = t + 1 - 2 * core
    split = kv_rows // piece
    q_pieces = q_rows // piece
    pieces = q_pieces + 2 * split
    count = 2 * pieces
    large = 2 * q_pieces
    shards_in_plane = tp_size * columns
    ranks = (t, other)

    def sequence(n):
        return n % 2 == 0, n // 2

    def row_of(index, m):
        if m < q_pieces:
            return pl.multiple_of(index * q_rows + m * piece, 8)
        m -= q_pieces
        base = shards_in_plane * (q_rows + (m // split) * kv_rows) + (m % split) * piece
        return pl.multiple_of(base + index * kv_rows, 8)

    def in_weights(at_column, at_side, n):
        own, m = sequence(n)
        of_core = core if own else 1 - core
        return weights.at[pl.ds(row_of(at_column * tp_size + at_side * 2 + of_core, m), piece)]

    def in_relay(n):
        return relay.at[pl.ds(n * piece, piece)]

    def in_shard(m):
        return shard.at[pl.ds(m * piece, piece)]

    def place(slot, n):
        return in_weights(column, side, n) if slot == 0 else in_relay(n)

    def twin_place(d, n):
        return in_weights((column - d) % columns, side, n)

    def remote(src, dst, send, recv, to_rep, to_tp):
        return pltpu.make_async_remote_copy(
            src_ref=src, dst_ref=dst, send_sem=send, recv_sem=recv,
            device_id=(to_rep, to_tp), device_id_type=MESH,
        )

    def inner(k):
        return (k > 0) & (k < planes - 1)

    def reached(k, at):
        return (at != k) & (inner(k) | (at == k + 1) | (at == k - 1))

    def beside(k, at):
        return ((k == 1) & (at == 0)) | ((k == planes - 2) & (at == planes - 1))

    def doubled(n, at):
        if n >= count - near:
            return reached(t, at)
        return reached(t, at) & jnp.logical_not(beside(t, at))

    def is_twice(n):
        return n >= count - twice

    def ups(slot):
        k = ranks[slot]
        return (plane >= k) & (plane < planes - 1), (plane <= k) & (plane > 0)

    def held_back(slot):
        k = ranks[slot]
        return (plane == k) & (k == planes - 2), (plane == k) & (k == 1)

    def late_sink(slot):
        k = ranks[slot]
        return ((plane == planes - 1) & (k == planes - 2)) | ((plane == 0) & (k == 1))

    def x_sends(n, src, dst, sem_of):
        for d in range(1, columns):
            to = plane * columns + (column + d) % columns
            remote(src, dst, x_send.at[d - 1], sem_of(d - 1), to, t).start()

    def forward(slot, n, src, source=False):
        up, down = ups(slot)
        if source:
            late_up, late_down = held_back(slot)
            up, down = up & jnp.logical_not(late_up), down & jnp.logical_not(late_down)
        dst = place(slot, n)

        @pl.when(up)
        def _():
            remote(src, dst, z_send.at[slot, 0], z_recv.at[slot, n], r + columns, t).start()

        @pl.when(down)
        def _():
            remote(src, dst, z_send.at[slot, 1], z_recv.at[slot, n], r - columns, t).start()

        if slot == 1:
            remote(src, in_weights(column, side, n), y_send.at[0], y_recv.at[n], r, other).start()
        elif not is_twice(n):
            x_sends(n, src, dst, lambda d: x_recv.at[d, 1 if n < large else 0])
        elif source:
            x_sends(n, src, dst, lambda d: pair_recv.at[d, n - (count - twice)])
        else:
            @pl.when(jnp.logical_not(doubled(n, plane)))
            def _():
                x_sends(n, src, dst, lambda d: x_recv.at[d, 3 if n < large else 4])

    def span(n):
        return weights.at[pl.ds(0, n * piece)]

    def recv_wait(dst, sem):
        remote(dst, dst, x_send.at[0], sem, r, partner).wait_recv()

    def send_wait(src, sem):
        remote(src, src, sem, x_recv.at[0, 0], r, partner).wait_send()

    def at_source(slot, n):
        own, m = sequence(n)
        return in_shard(m) if own else place(slot, n)

    taken = [0, 0]

    def take(slot, n):
        while taken[slot] <= n:
            own, m = sequence(taken[slot])
            if not own:
                @pl.when(plane == ranks[slot])
                def _():
                    recv_wait(place(slot, taken[slot]), part_recv.at[m])
            taken[slot] += 1

    def source_step(slot, n):
        take(slot, n)

        @pl.when(plane == ranks[slot])
        def _():
            forward(slot, n, at_source(slot, n), True)

    def late_step(slot, n):
        take(slot, n)
        if slot == 1 and n < CROSS:
            return
        late_up, late_down = held_back(slot)
        src, dst = at_source(slot, n), place(slot, n)

        @pl.when(late_up)
        def _():
            remote(src, dst, z_send.at[slot, 0], z_recv.at[slot, n], r + columns, t).start()

        @pl.when(late_down)
        def _():
            remote(src, dst, z_send.at[slot, 1], z_recv.at[slot, n], r - columns, t).start()

    def relay_step(slot, n, late):
        sink = late_sink(slot)
        if slot == 1 and late and n < CROSS:
            return

        @pl.when((plane != ranks[slot]) & (sink if late else jnp.logical_not(sink)))
        def _():
            recv_wait(place(slot, n), z_recv.at[slot, n])
            forward(slot, n, place(slot, n))

    def y_step(n, late):
        sink = late_sink(0)

        @pl.when(sink if late else jnp.logical_not(sink))
        def _():
            block = in_weights(column, 1 - side, n)
            recv_wait(block, cross_recv.at[n] if late and n < CROSS else y_recv.at[n])
            x_sends(n, block, block, lambda d: x_recv.at[d, 2 if n < large else 0])
            if n < CROSS and not late:
                @pl.when((plane == t) & (t == 1))
                def _():
                    remote(block, block, cross_send.at[0], cross_recv.at[n], r - columns, t).start()

                @pl.when((plane == t) & (t == planes - 2))
                def _():
                    remote(block, block, cross_send.at[0], cross_recv.at[n], r + columns, t).start()

    def goes_up(n):
        return (plane >= t) & (plane < planes - 1) & doubled(n, plane + 1)

    def goes_down(n):
        return (plane <= t) & (plane > 0) & doubled(n, plane - 1)

    def goes(n):
        return goes_up(n) | goes_down(n)

    def twin_step(d, n, source):
        src = twin_place(d, n)
        at = n - (count - twice)
        here = plane == t if source else (plane != t) & goes(n)

        @pl.when(here)
        def _():
            recv_wait(src, pair_recv.at[d - 1, at] if source else twin_recv.at[d - 1, at])

        @pl.when(here & goes_up(n))
        def _():
            remote(src, src, twin_send.at[0], twin_recv.at[d - 1, at], r + columns, t).start()

        @pl.when(here & goes_down(n))
        def _():
            remote(src, src, twin_send.at[1], twin_recv.at[d - 1, at], r - columns, t).start()

    def twin_sink(d, n):
        @pl.when(doubled(n, plane) & jnp.logical_not(goes(n)))
        def _():
            recv_wait(twin_place(d, n), twin_recv.at[d - 1, n - (count - twice)])

    handler = core == plane % 2
    rows = tok.shape[0]
    chunk = rows // TOK_CHUNKS

    def prompt_rows(rank):
        return prompts.at[pl.ds(pl.multiple_of(rank * rows, 8), rows)]

    def prompt_chunk(rank, i):
        return prompts.at[pl.ds(pl.multiple_of(rank * rows + i * chunk, 8), chunk)]

    barrier = pltpu.get_barrier_semaphore()

    def greet(to_rep, to_tp):
        pl.semaphore_signal(barrier, inc=1, device_id=(to_rep, to_tp), device_id_type=MESH)

    @pl.when(plane < planes - 1)
    def _():
        greet(r + columns, t)

    @pl.when(plane > 0)
    def _():
        greet(r - columns, t)

    for d in range(1, columns):
        greet(plane * columns + (column + d) % columns, t)
    greet(r, other)
    greet(r, partner)

    chunks = q_rows // kv_rows
    loads = [
        pltpu.make_async_copy(
            q_weight.at[pl.ds(i * kv_rows, kv_rows)], wide.at[pl.ds(i * kv_rows, kv_rows)], load_sem.at[i]
        )
        for i in range(chunks)
    ] + [
        pltpu.make_async_copy(w, wide.at[pl.ds(q_rows + i * kv_rows, kv_rows)], load_sem.at[chunks + i])
        for i, w in enumerate((k_weight, v_weight))
    ]
    load_tok = pltpu.make_async_copy(tok, prompt_rows(t), local_sem.at[0])
    for load in loads:
        load.start()
    load_tok.start()

    def cast(m):
        at = pl.ds(m * piece, piece)
        value = wide[at, :].astype(shard.dtype)
        shard[at, :] = value

        @pl.when(plane == t)
        def _():
            weights[pl.ds(row_of(column * tp_size + t, m), piece), :] = value

    def part(m):
        @pl.when(jnp.logical_not(handler))
        def _():
            @pl.when(side == plane // 2)
            def _():
                dst = weights.at[pl.ds(row_of(column * tp_size + t, m), piece)]
                remote(in_shard(m), dst, part_send.at[0], part_recv.at[m], r, partner).start()

            @pl.when(side != plane // 2)
            def _():
                remote(in_shard(m), in_relay(2 * m + 1), part_send.at[0], part_recv.at[m], r, partner).start()

    loads[0].wait()
    for m in range(split):
        cast(m)
    neighbours = columns + 1 + jnp.where(inner(plane), 2, 1)
    pl.semaphore_wait(barrier, neighbours)
    for m in range(split):
        part(m)
    lead = min(LEAD, 2 * split)
    for n in range(lead):
        source_step(0, n)
        source_step(1, n)
    for i in range(1, chunks + 2):
        loads[i].wait()
        for m in range(i * split, (i + 1) * split):
            cast(m)
            part(m)
    for n in range(lead, LEAD):
        source_step(0, n)
        source_step(1, n)
    load_tok.wait()
    remote(tok, prompt_rows(t), tok_send.at[1], tok_recv.at[1], r, partner).start()

    late, sunk, late_y, sent, twins, far = [0, 0], [0, 0], 0, 0, 0, 0
    pairs = [(d, n) for n in range(count - twice, count) for d in range(1, columns)]
    block = shards_in_plane * kv_rows
    blocks, own_blocks = order_of(columns, tp_size, q_rows, kv_rows, column)

    def late_to(slot, stop):
        while late[slot] < min(stop, count):
            late_step(slot, late[slot])
            late[slot] += 1

    def sink_to(slot, stop):
        while sunk[slot] < min(stop, count):
            relay_step(slot, sunk[slot], True)
            sunk[slot] += 1

    def late_y_to(stop):
        nonlocal late_y
        while late_y < min(stop, count):
            y_step(late_y, True)
            late_y += 1

    def send_tokens(stop):
        nonlocal sent
        while sent < min(stop, TOK_CHUNKS):
            at = pl.ds(sent * chunk, chunk)
            remote(tok.at[at], prompt_chunk(t, sent), tok_send.at[0], tok_recv.at[0], r, other).start()
            sent += 1

    def twins_to(stop):
        nonlocal twins
        while twins < min(stop, len(pairs)):
            twin_step(*pairs[twins], True)
            twins += 1

    def far_to(stop):
        nonlocal far
        while far < min(stop, len(pairs)):
            twin_step(*pairs[far], False)
            far += 1

    def meet():
        send_tokens(TOK_CHUNKS)
        recv_wait(prompt_rows(other), tok_recv.at[0])
        remote(prompt_rows(other), prompt_rows(other), tok_send.at[2], tok_recv.at[2], r, partner).start()

    def begin():
        recv_wait(prompt_rows(partner), tok_recv.at[1])
        recv_wait(prompt_rows((partner + half) % tp_size), tok_recv.at[2])

    def arrive(first, stop, sems):
        plain = max(min(stop, count - twice) - first, 0)
        extra = stop - first - plain
        for d in range(1, columns):
            if sems[0] != sems[1]:
                if plain:
                    recv_wait(span(plain), x_recv.at[d - 1, sems[0]])
                recv_wait(span(stop - first), x_recv.at[d - 1, sems[1]])
            else:
                recv_wait(span(plain + stop - first), x_recv.at[d - 1, sems[0]])
            if extra:
                @pl.when((plane != t) & jnp.logical_not(reached(t, plane)))
                def _():
                    recv_wait(span(extra), x_recv.at[d - 1, sems[2]])
            single = max(min(stop, count - near) - max(first, count - twice), 0)
            if single:
                @pl.when(beside(t, plane))
                def _():
                    recv_wait(span(single), x_recv.at[d - 1, sems[2]])
        for d, n in pairs:
            if first <= n < stop:
                twin_sink(d, n)

    send_tokens(TOK_FIRST)
    for slot in range(2):
        late_to(slot, LATE_FIRST[slot])
    for n in range(count):
        for slot in range(2):
            late_to(slot, LATE_FIRST[slot] + (n + 1) * LATE_RATE[slot] // 4)
        if n + LEAD < count:
            source_step(0, n + LEAD)
            source_step(1, n + LEAD)
        relay_step(0, n, False)
        relay_step(1, n, False)
        for slot in range(2):
            sink_to(slot, (n + 1) * LATE_RATE[slot] // 4)
        if n >= TOK_AT:
            send_tokens(TOK_FIRST + (n - TOK_AT) * TOK_RATE // 4 + 1)
        if n >= Y_LAG:
            y_step(n - Y_LAG, False)
        late_y_to((n + 1) * min(LATE_RATE) // 4 - Y_LAG)
        if twice and n >= TWIN_AT:
            twins_to((n - TWIN_AT) * TWIN_RATE // 4 + 1)
        if twice and n >= FAR_AT:
            far_to((n - FAR_AT) * TWIN_RATE // 4 + 1)
        if n == MEET_AT:
            meet()
    for slot in range(2):
        late_to(slot, count)
    for n in range(count - Y_LAG, count):
        y_step(n, False)
    if MEET_AT >= count:
        meet()
    begin()
    twins_to(len(pairs))
    done = 0

    def multiply_to(stop):
        nonlocal done
        while done < stop:
            if done == own_blocks:
                arrive(0, large, (1, 2, 3))
            multiply(blocks[done], prompts, weights, projected, None, block)
            done += 1

    for slot in range(2):
        sink_to(slot, count)
    late_y_to(count)
    for i in range(len(pairs)):
        far_to(i + 1)
        multiply_to(sum(i >= at for at in BLOCK_AT[:own_blocks]))
    multiply_to(len(blocks) - 2)
    arrive(large, count, (0, 0, 4))

    def sent_when(go, n, sem):
        if n:
            @pl.when(go)
            def _():
                send_wait(span(n), sem)

    for d in range(1, columns):
        send_wait(span(2 * count - twice), x_send.at[d - 1])
        sent_when(jnp.logical_not(reached(t, plane)), twice, x_send.at[d - 1])
        sent_when(beside(t, plane), twice - near, x_send.at[d - 1])
    send_wait(span(count - CROSS), y_send.at[0])
    sent_when(jnp.logical_not(late_sink(1)), CROSS, y_send.at[0])
    for slot in range(2):
        for way in range(2):
            go, held = ups(slot)[way], held_back(slot)[way]
            sent_when(go, count - CROSS, z_send.at[slot, way])
            sent_when(go & jnp.logical_not(held) if slot else go, CROSS, z_send.at[slot, way])
    if twice:
        for way, go in enumerate((goes_up, goes_down)):
            sent_when(go(count - 1), near * (columns - 1), twin_send.at[way])
            sent_when(go(count - twice), (twice - near) * (columns - 1), twin_send.at[way])
    sent_when((plane == t) & inner(t), CROSS, cross_send.at[0])

    @pl.when(jnp.logical_not(handler))
    def _():
        send_wait(shard, part_send.at[0])

    for i in range(3):
        send_wait(tok, tok_send.at[i])


def shards(q_weight, key_projection_weight, value_projection_weight, tokens):
    rep_size, tp_size = lax.axis_size("rep"), lax.axis_size("tp")
    columns = rep_size // tp_size
    q_rows, width = q_weight.shape
    kv_rows = key_projection_weight.shape[0]
    piece = kv_rows // 2 if kv_rows % 32 == 0 else kv_rows
    pieces = (q_rows + 2 * kv_rows) // piece
    count = 2 * pieces
    twice, near = [count * a // b if columns == 2 else 0 for a, b in (TWICE, NEAR)]
    hbm = pl.BlockSpec(memory_space=pltpu.HBM)
    dma = pltpu.SemaphoreType.DMA
    dtype = tokens.dtype
    block = columns * tp_size * kv_rows
    rows = tp_size * tokens.shape[0]
    each = q_rows + 2 * kv_rows
    total = columns * tp_size * each
    vmem = pl.BlockSpec(memory_space=pltpu.VMEM)
    inputs = [
        pltpu.with_memory_space_constraint(a, pltpu.HBM)
        for a in (q_weight, key_projection_weight, value_projection_weight, tokens)
    ]
    held = pl.pallas_call(
        functools.partial(gather_kernel, rep_size, tp_size, q_rows, kv_rows, piece, twice, near),
        out_shape=(
            pltpu.VMEM((total, width), dtype),
            pltpu.VMEM((rows, width), dtype),
            pltpu.VMEM((rows, total), dtype),
        ),
        in_specs=[hbm] * 4,
        out_specs=(vmem,) * 3,
        scratch_shapes=[
            pltpu.VMEM((count * piece, width), dtype),
            pltpu.VMEM((each, width), dtype),
            pltpu.VMEM((each, width), q_weight.dtype),
            dma((q_rows // kv_rows + 2,)), dma((1,)),
            dma((1,)), dma((pieces,)),
            dma((2, 2)), dma((2, count)),
            dma((1,)), dma((count,)),
            dma((columns - 1,)), dma((columns - 1, 5)),
            dma((3,)), dma((3,)),
            dma((columns - 1, max(twice, 1))), dma((2,)), dma((columns - 1, max(twice, 1))),
            dma((1,)), dma((max(CROSS, 1),)),
        ],
        compiler_params=pltpu.CompilerParams(
            has_side_effects=True, collective_id=0, vmem_limit_bytes=VMEM * 2**20
        ),
    )(*inputs)
    blocks = total // block
    return pl.pallas_call(
        functools.partial(finish_kernel, columns, tp_size, q_rows, kv_rows),
        out_shape=(
            jax.ShapeDtypeStruct((total, width), dtype),
            jax.ShapeDtypeStruct((rows, total), dtype),
        ),
        in_specs=[vmem] * 3,
        out_specs=(hbm, hbm),
        scratch_shapes=[
            pltpu.VMEM((rows, 2 * block), dtype), dma((blocks,)), dma((blocks,)), dma((2,)),
        ],
        compiler_params=pltpu.CompilerParams(vmem_limit_bytes=VMEM * 2**20),
    )(*held)


def solution(mesh):
    spec = P(("rep", "tp"), None)
    return jax.shard_map(
        shards, mesh=mesh, in_specs=(spec,) * 4, out_specs=(P("tp", None), P("rep", "tp")), check_vma=False
    )
```
